32 devices in a mesh: cohort: 2 (over x), tile: 16 (over z, y, core).
Axes of the slice: x: 2, y: 2, z: 4, core: 2. Of those that a mesh axis runs over, the one named last changes fastest.
Arguments:
- dosage: bfloat16 [512, 8192], P(('cohort', 'tile')), parts along dimension 0, may hold values from 0 to 2
- covars: float32 [512, 16], P(('cohort', 'tile')), parts along dimension 0, may hold values from -12 to 12, as said below
- phenotypes: float32 [512, 1792], P(('cohort', 'tile')), parts along dimension 0, may hold values from -100 to 100
Outputs:
- mean_chi: float32 [3584], P(('cohort', 'tile')), parts along dimension 0
- hit_rate: float32 [3584], P(('cohort', 'tile')), parts along dimension 0
The draws below stay inside these ranges and needn't reach their ends.
There are 2 independent parts, one for each index of `cohort`. The reference program is written for one: setup_inputs(seed, part) draws one part's arguments, and reference() takes and returns one part's arrays. A program takes and returns all parts, laid end to end along the dimension named above; each array names one. Nothing has to cross between parts.
Inputs may be any that keep to these rules, and one draw needn't show every extreme that they name: `covars`: each covariate column has its own mean and spread.
All inputs are finite; a program needn't handle non-finite values.
Results may differ from the reference program's by a relative error of at most 0.003.
Values may be sent and summed in bfloat16 or wider, within the bound.
A program may use at most 64 MiB of HBM per device.

```python
import math
import jax
import jax.numpy as jnp
from jax import lax

VARIANTS = 8192
COVS = 16
SAMPLES = 256
GENES = 1792


def ancestry_score(key):
    label = (jax.random.uniform(jax.random.fold_in(key, 14), (SAMPLES,), jnp.float32) < 0.4).astype(jnp.float32)
    blur = jnp.clip(jax.random.normal(jax.random.fold_in(key, 15), (SAMPLES,), jnp.float32), -4.0, 4.0)
    return label + 0.15 * blur


def covar_table(key):
    base = jnp.clip(jax.random.normal(jax.random.fold_in(key, 11), (SAMPLES, COVS), jnp.float32), -5.0, 5.0)
    score = 2.0 * ancestry_score(key) - 1.0
    base = jnp.concatenate([score[:, None], base[:, 1:]], axis=1)
    means = jax.random.uniform(jax.random.fold_in(key, 12), (COVS,), jnp.float32, -2.0, 2.0)
    spread = jnp.exp(jax.random.uniform(jax.random.fold_in(key, 13), (COVS,), jnp.float32, math.log(0.5), math.log(2.0)))
    return base * spread[None, :] + means[None, :]


def draw_covars(key, part):
    return covar_table(key)


def draw_dosage(key, part):
    score = ancestry_score(key)
    base_freq = jax.random.uniform(jax.random.fold_in(key, 31), (VARIANTS,), jnp.float32, 0.05, 0.95)
    shift = jax.random.uniform(jax.random.fold_in(key, 32), (VARIANTS,), jnp.float32, -0.4, 0.4)
    freq = jnp.clip(base_freq[None, :] + shift[None, :] * (score[:, None] - 0.5), 0.02, 0.98)
    first = (jax.random.uniform(jax.random.fold_in(key, 33), (SAMPLES, VARIANTS), jnp.float32) < freq).astype(jnp.float32)
    second = (jax.random.uniform(jax.random.fold_in(key, 34), (SAMPLES, VARIANTS), jnp.float32) < freq).astype(jnp.float32)
    blur = 0.2 * jnp.clip(jax.random.normal(jax.random.fold_in(key, 35), (SAMPLES, VARIANTS), jnp.float32), -3.0, 3.0)
    return jnp.clip(first + second + blur, 0.0, 2.0).astype(jnp.bfloat16)


def draw_phenotypes(key, part):
    table = covar_table(key)
    effect = jnp.clip(jax.random.normal(jax.random.fold_in(key, 21), (COVS, GENES), jnp.float32), -4.0, 4.0)
    spread = jnp.exp(jax.random.uniform(jax.random.fold_in(key, 22), (GENES,), jnp.float32, math.log(0.5), math.log(2.0)))
    noise = jnp.clip(jax.random.normal(jax.random.fold_in(key, 23), (SAMPLES, GENES), jnp.float32), -8.0, 8.0) * spread[None, :]
    signal = jnp.dot(table, effect, precision=lax.Precision.HIGHEST)
    return jnp.clip(signal + noise, -100.0, 100.0)


def setup_inputs(seed: int = 0, part: int = 0) -> dict:
    streams_of = jax.random.split(jax.random.key(seed), 4)
    own_keys = jax.random.split(jax.random.fold_in(streams_of[3], part), 4)
    dosage = draw_dosage(jax.random.fold_in(jax.random.fold_in(streams_of[3], part), 71), part)
    covars = draw_covars(jax.random.fold_in(jax.random.fold_in(streams_of[3], part), 71), part)
    phenotypes = draw_phenotypes(jax.random.fold_in(jax.random.fold_in(streams_of[3], part), 71), part)
    return dict(dosage=dosage, covars=covars, phenotypes=phenotypes)


def reference(dosage, covars, phenotypes):
    highest = lax.Precision.HIGHEST
    dose_real = dosage.astype(jnp.float32)
    samples = dose_real.shape[0]
    variants = dose_real.shape[1]
    gram = jnp.dot(covars.T.astype(jnp.float32), covars.astype(jnp.float32), precision=highest, preferred_element_type=jnp.float32)
    cov_dose = jnp.dot(covars.T.astype(jnp.float32), dose_real.astype(jnp.float32), precision=highest, preferred_element_type=jnp.float32)
    cov_pheno = jnp.dot(covars.T.astype(jnp.float32), phenotypes.astype(jnp.float32), precision=highest, preferred_element_type=jnp.float32)
    factor = jnp.linalg.cholesky(gram)
    betas = jax.scipy.linalg.cho_solve((factor, True), jnp.concatenate([cov_dose, cov_pheno], axis=1))
    beta_dose = betas[:, :variants]
    beta_pheno = betas[:, variants:]
    dose_resid = dose_real - jnp.dot(covars.astype(jnp.float32), beta_dose.astype(jnp.float32), precision=highest, preferred_element_type=jnp.float32)
    pheno_resid = phenotypes - jnp.dot(covars.astype(jnp.float32), beta_pheno.astype(jnp.float32), precision=highest, preferred_element_type=jnp.float32)
    dose_sumsq = lax.optimization_barrier(jnp.sum(dose_resid * dose_resid, axis=0))
    pheno_sumsq = lax.optimization_barrier(jnp.sum(pheno_resid * pheno_resid, axis=0))
    dose_bf = dose_resid.astype(jnp.bfloat16)
    pheno_bf = pheno_resid.astype(jnp.bfloat16)
    cross = lax.dot_general(pheno_bf.astype(jnp.float32), dose_bf.astype(jnp.float32), (((0,), (0,)), ((), ())), preferred_element_type=jnp.float32)
    dose_var = dose_sumsq / samples + 0.1
    pheno_var = pheno_sumsq / samples + 0.1
    zscore = cross / (jnp.sqrt(jnp.float32(samples)) * jnp.sqrt(pheno_var[:, None] * dose_var[None, :]))
    chi_square = zscore * zscore
    mean_chi = lax.optimization_barrier(jnp.mean(chi_square, axis=1))
    hit_rate = 20.0 / variants * lax.optimization_barrier(jnp.sum(jax.nn.sigmoid(2.0 * (chi_square - 4.0)), axis=1))
    return (mean_chi, hit_rate)
```

```python
import functools

import jax
import jax.numpy as jnp
from jax import lax
from jax.experimental import pallas as pl
from jax.experimental.pallas import tpu as pltpu
from jax.sharding import PartitionSpec as P

LANES = 128
HIGH = lax.Precision.HIGHEST


def dot(a, b, ca, cb, precision=HIGH):
    return lax.dot_general(
        a, b, (((ca,), (cb,)), ((), ())), precision=precision, preferred_element_type=jnp.float32
    )


def inverse(gram):
    size = gram.shape[0]
    row_id = lax.broadcasted_iota(jnp.int32, (size, 2 * size), 0)
    eye = (
        lax.broadcasted_iota(jnp.int32, (size, size), 0)
        == lax.broadcasted_iota(jnp.int32, (size, size), 1)
    ).astype(jnp.float32)
    work = jnp.concatenate([gram, eye], axis=1)
    for k in range(size):
        row = work[k : k + 1, :] / work[k : k + 1, k : k + 1]
        work = jnp.where(row_id == k, row, work - work[:, k : k + 1] * row)
    return work[:, size:]


def kernel(
    n, zs, ys, cs, own,
    dose_ref, cov_ref, pheno_ref, out_ref,
    cov_all, raw, dose_all, blocks, doset, scale, part, landed,
    cov_send, cov_recv, raw_send, raw_recv, dose_send, dose_recv,
    z_send, y_send, c_send, blk_recv, part_send, part_recv,
):
    me = lax.axis_index("tile")
    rows, variants = dose_ref.shape
    covs = cov_ref.shape[1]
    genes = pheno_ref.shape[1]
    nb = genes // LANES
    width = variants // n
    samples = rows * n
    c = lax.rem(me, cs)
    y = lax.rem(me // cs, ys)
    z = me // (cs * ys)

    def index(zi, yi, ci):
        return (zi * ys + yi) * cs + ci

    def remote(src, dst, ssem, rsem, dev):
        return pltpu.make_async_remote_copy(
            src_ref=src, dst_ref=dst, send_sem=ssem, recv_sem=rsem,
            device_id={"tile": dev}, device_id_type=pl.DeviceIdType.MESH,
        )

    def row_slice(t):
        return pl.ds(pl.multiple_of(t * rows, rows), rows)

    def lane_slice(start, size):
        return pl.ds(pl.multiple_of(start, LANES), size)

    barrier = pltpu.get_barrier_semaphore()
    for k in range(1, n):
        pl.semaphore_signal(
            barrier, inc=1, device_id={"tile": lax.rem(me + k, n)},
            device_id_type=pl.DeviceIdType.MESH,
        )
    pl.semaphore_wait(barrier, n - 1)

    def cov_copy(src, dev):
        return remote(cov_ref, cov_all.at[row_slice(src), :], cov_send.at[dev], cov_recv.at[src], dev)

    def raw_copy(src, dev):
        return remote(
            pheno_ref.at[:, lane_slice(dev * LANES, LANES)],
            raw.at[row_slice(src), :], raw_send.at[dev], raw_recv.at[src], dev,
        )

    def dose_copy(src, dev):
        return remote(
            dose_ref.at[:, lane_slice(dev * width, width)],
            dose_all.at[row_slice(src), :], dose_send.at[dev], dose_recv.at[src], dev,
        )

    def others(body):
        @pl.loop(1, n)
        def _(k):
            body(lax.rem(me + k, n))

    def send_first(dev):
        cov_copy(me, dev).start()

        @pl.when(dev < nb)
        def _():
            raw_copy(me, dev).start()

    others(send_first)
    others(lambda dev: dose_copy(me, dev).start())

    cov_all[row_slice(me), :] = cov_ref[...]
    dose_all[row_slice(me), :] = dose_ref[:, lane_slice(me * width, width)]

    others(lambda src: cov_copy(src, me).wait_recv())
    cov = cov_all[...]
    eye = (
        lax.broadcasted_iota(jnp.int32, (covs, covs), 0)
        == lax.broadcasted_iota(jnp.int32, (covs, covs), 1)
    ).astype(jnp.float32)
    covt = dot(eye, cov, 1, 1)
    solve = dot(cov, inverse(dot(covt, cov, 1, 0)), 1, 0)

    def blk_z(o, dev):
        return remote(blocks.at[o], blocks.at[o], z_send.at[dev // (cs * ys)], blk_recv.at[o], dev)

    def blk_y(o, dev):
        return remote(blocks.at[o], blocks.at[o], y_send.at[o], blk_recv.at[o], dev)

    def blk_c(o, dev):
        return remote(blocks.at[o], blocks.at[o], c_send.at[o], blk_recv.at[o], dev)

    y_dev = index(z, lax.rem(y + 1, ys), c)
    c_dev = index(z, y, lax.rem(c + 1, cs))

    @pl.when(me < nb)
    def _():
        raw[row_slice(me), :] = pheno_ref[:, lane_slice(me * LANES, LANES)]
        others(lambda src: raw_copy(src, me).wait_recv())
        pheno = raw[...]
        resid = pheno - dot(solve, dot(covt, pheno, 1, 0), 1, 0)
        var = jnp.sum(resid * resid, axis=0, keepdims=True) / samples + 0.1
        inv = 1.0 / var
        hi = inv.astype(jnp.bfloat16)
        rest = inv - hi.astype(jnp.float32)
        mid = rest.astype(jnp.bfloat16)
        low = (rest - mid.astype(jnp.float32)).astype(jnp.bfloat16)
        line = lax.broadcasted_iota(jnp.int32, (16, LANES), 0)
        extra = jnp.where(
            line == 0, hi.astype(jnp.float32),
            jnp.where(line == 1, mid.astype(jnp.float32),
                      jnp.where(line == 2, low.astype(jnp.float32), 0.0)),
        )
        blocks[me, pl.ds(samples, 16), :] = extra.astype(jnp.bfloat16)
        blocks[me, pl.ds(0, samples), :] = resid.astype(jnp.bfloat16)
        for k in range(1, zs):
            blk_z(me, index(lax.rem(z + k, zs), y, c)).start()
        if ys > 1:
            blk_y(me, y_dev).start()
        if cs > 1:
            blk_c(me, c_dev).start()

    others(lambda src: dose_copy(src, me).wait_recv())
    dose = dose_all[...].astype(jnp.float32).T
    dose = dose - dot(dot(dose, cov, 1, 0), solve, 1, 1)
    doset[...] = dose.astype(jnp.bfloat16)
    dose_var = jnp.sum(dose * dose, axis=1, keepdims=True) / samples + 0.1
    scale[...] = jnp.broadcast_to(1.0 / (samples * dose_var), scale.shape)

    def compute(o):
        extra = blocks[o, pl.ds(samples, 16), :].astype(jnp.float32)
        gene_scale = jnp.sum(extra[0:3, :], axis=0, keepdims=True)
        cross = dot(doset[...], blocks[o, pl.ds(0, samples), :], 1, 0, None)
        chi = cross * cross * (scale[...] * gene_scale)
        hit = 1.0 / (1.0 + jnp.exp(-2.0 * (chi - 4.0)))
        cols = lane_slice(o * LANES, LANES)
        part[0:1, cols] = jnp.sum(chi, axis=0, keepdims=True)
        part[1:2, cols] = jnp.sum(hit, axis=0, keepdims=True)

    @pl.when(me < nb)
    def _():
        compute(me)

    @pl.loop(1, zs)
    def _(k):
        o = index(lax.rem(z + k, zs), y, c)

        @pl.when(o < nb)
        def _():
            blk_z(o, me).wait_recv()
            if ys > 1:
                blk_y(o, y_dev).start()
            if cs > 1:
                blk_c(o, c_dev).start()
            compute(o)

    if ys > 1:
        @pl.loop(0, zs)
        def _(k):
            o = index(lax.rem(z + k, zs), lax.rem(y + 1, ys), c)

            @pl.when(o < nb)
            def _():
                blk_y(o, me).wait_recv()
                if cs > 1:
                    blk_c(o, c_dev).start()
                compute(o)

    if cs > 1:
        for j in range(ys):
            @pl.loop(0, zs)
            def _(k):
                o = index(lax.rem(z + k, zs), lax.rem(y + j, ys), lax.rem(c + 1, cs))

                @pl.when(o < nb)
                def _():
                    blk_c(o, me).wait_recv()
                    compute(o)

    window = landed.shape[2]

    def first(dev):
        return jnp.minimum(own * dev // LANES * LANES, genes - window)

    def part_copy(src, dev):
        return remote(
            part.at[:, lane_slice(first(dev), window)], landed.at[src],
            part_send.at[dev], part_recv.at[src], dev,
        )

    others(lambda dev: part_copy(me, dev).start())
    landed[me] = part[:, lane_slice(first(me), window)]
    others(lambda src: part_copy(src, me).wait_recv())
    total = jnp.sum(landed[...], axis=0)
    shift = own * me - first(me)
    out_ref[...] = pltpu.roll(total, lax.rem(window - shift, window), 1)

    def drain(dev):
        cov_copy(me, dev).wait_send()
        dose_copy(me, dev).wait_send()
        part_copy(me, dev).wait_send()

        @pl.when(dev < nb)
        def _():
            raw_copy(me, dev).wait_send()

    others(drain)

    @pl.when(me < nb)
    def _():
        for k in range(1, zs):
            blk_z(me, index(lax.rem(z + k, zs), y, c)).wait_send()

    @pl.loop(0, zs)
    def _(k):
        o = index(lax.rem(z + k, zs), y, c)

        @pl.when(o < nb)
        def _():
            if ys > 1:
                blk_y(o, y_dev).wait_send()
            if cs > 1:
                blk_c(o, c_dev).wait_send()

        if ys > 1 and cs > 1:
            other = index(lax.rem(z + k, zs), lax.rem(y + 1, ys), c)

            @pl.when(other < nb)
            def _():
                blk_c(other, c_dev).wait_send()


def local(dosage, covars, phenotypes):
    n = lax.axis_size("tile")
    rows, variants = dosage.shape
    genes = phenotypes.shape[1]
    covs = covars.shape[1]
    samples = rows * n
    cs = 2 if n % 2 == 0 else 1
    ys = 2 if n % (2 * cs) == 0 else 1
    zs = n // (cs * ys)
    nb = genes // LANES
    own = genes // n
    width = variants // n
    window = (own + LANES - 1 + LANES - 1) // LANES * LANES
    dma = pltpu.SemaphoreType.DMA
    out = pl.pallas_call(
        functools.partial(kernel, n, zs, ys, cs, own),
        out_shape=jax.ShapeDtypeStruct((8, window), jnp.float32),
        in_specs=[pl.BlockSpec(memory_space=pltpu.VMEM)] * 3,
        out_specs=pl.BlockSpec(memory_space=pltpu.VMEM),
        scratch_shapes=[
            pltpu.VMEM((samples, covs), jnp.float32),
            pltpu.VMEM((samples, LANES), jnp.float32),
            pltpu.VMEM((samples, width), jnp.bfloat16),
            pltpu.VMEM((nb, samples + 16, LANES), jnp.bfloat16),
            pltpu.VMEM((width, samples), jnp.bfloat16),
            pltpu.VMEM((width, LANES), jnp.float32),
            pltpu.VMEM((8, genes), jnp.float32),
            pltpu.VMEM((n, 8, window), jnp.float32),
            dma((n,)), dma((n,)), dma((n,)), dma((n,)), dma((n,)), dma((n,)),
            dma((zs,)), dma((nb,)), dma((nb,)), dma((nb,)), dma((n,)), dma((n,)),
        ],
        compiler_params=pltpu.CompilerParams(collective_id=0, has_side_effects=True),
    )(dosage, covars, phenotypes)
    return out[0, :own] / variants, 20.0 / variants * out[1, :own]


def solution(mesh):
    spec = P(("cohort", "tile"), None)
    return jax.shard_map(
        local,
        mesh=mesh,
        in_specs=(spec, spec, spec),
        out_specs=(P(("cohort", "tile")), P(("cohort", "tile"))),
        check_vma=False,
    )
```

```python
import functools

import jax
import jax.numpy as jnp
from jax import lax
from jax.experimental import pallas as pl
from jax.experimental.pallas import tpu as pltpu
from jax.sharding import PartitionSpec as P

LANES = 128
HIGH = lax.Precision.HIGHEST


def dot(a, b, ca, cb, precision=HIGH):
    return lax.dot_general(
        a, b, (((ca,), (cb,)), ((), ())), precision=precision, preferred_element_type=jnp.float32
    )


def inverse(gram):
    size = gram.shape[0]
    row_id = lax.broadcasted_iota(jnp.int32, (size, 2 * size), 0)
    eye = (
        lax.broadcasted_iota(jnp.int32, (size, size), 0)
        == lax.broadcasted_iota(jnp.int32, (size, size), 1)
    ).astype(jnp.float32)
    work = jnp.concatenate([gram, eye], axis=1)
    for k in range(size):
        row = work[k : k + 1, :] / work[k : k + 1, k : k + 1]
        work = jnp.where(row_id == k, row, work - work[:, k : k + 1] * row)
    return work[:, size:]


def kernel(
    n, zs, ys, cs, own,
    dose_ref, cov_ref, pheno_ref, out_ref,
    cov_all, raw, dose_all, blocks, doset, scale, part, landed,
    cov_own, cov_send, cov_recv, raw_send, raw_recv, dose_send, dose_recv,
    z_send, y_send, c_send, blk_recv, part_send, part_recv,
):
    me = lax.axis_index("tile")
    rows, variants = dose_ref.shape
    covs = cov_ref.shape[1]
    genes = pheno_ref.shape[1]
    nb = genes // LANES
    width = variants // n
    samples = rows * n
    c = lax.rem(me, cs)
    y = lax.rem(me // cs, ys)
    z = me // (cs * ys)

    def index(zi, yi, ci):
        return (zi * ys + yi) * cs + ci

    def remote(src, dst, ssem, rsem, dev):
        return pltpu.make_async_remote_copy(
            src_ref=src, dst_ref=dst, send_sem=ssem, recv_sem=rsem,
            device_id={"tile": dev}, device_id_type=pl.DeviceIdType.MESH,
        )

    def row_slice(t):
        return pl.ds(pl.multiple_of(t * rows, rows), rows)

    def lane_slice(start, size):
        return pl.ds(pl.multiple_of(start, LANES), size)

    groups = rows // 8
    packed = [cov_ref[8 * g : 8 * g + 8, :] for g in range(groups)]
    fill = jnp.zeros((8, LANES - groups * covs), jnp.float32)
    cov_own[...] = jnp.concatenate(packed + [fill], axis=1)

    barrier = pltpu.get_barrier_semaphore()
    for k in range(1, n):
        pl.semaphore_signal(
            barrier, inc=1, device_id={"tile": lax.rem(me + k, n)},
            device_id_type=pl.DeviceIdType.MESH,
        )
    pl.semaphore_wait(barrier, n - 1)

    def cov_copy(src, dev):
        return remote(cov_own, cov_all.at[src], cov_send.at[dev], cov_recv.at[src], dev)

    def raw_copy(src, dev):
        return remote(
            pheno_ref.at[:, lane_slice(dev * LANES, LANES)],
            raw.at[row_slice(src), :], raw_send.at[dev], raw_recv.at[src], dev,
        )

    def dose_copy(src, dev):
        return remote(
            dose_ref.at[:, lane_slice(dev * width, width)],
            dose_all.at[row_slice(src), :], dose_send.at[dev], dose_recv.at[src], dev,
        )

    def others(body):
        @pl.loop(1, n)
        def _(k):
            body(lax.rem(me + k, n))

    others(lambda dev: cov_copy(me, dev).start())

    def send_first(dev):
        @pl.when(dev < nb)
        def _():
            raw_copy(me, dev).start()

    others(send_first)
    others(lambda dev: dose_copy(me, dev).start())

    cov_all[me] = cov_own[...]
    dose_all[row_slice(me), :] = dose_ref[:, lane_slice(me * width, width)]

    others(lambda src: cov_copy(src, me).wait_recv())
    tiles = cov_all[...]
    cov = jnp.concatenate(
        [tiles[:, :, g * covs : (g + 1) * covs] for g in range(groups)], axis=1
    ).reshape(samples, covs)
    eye = (
        lax.broadcasted_iota(jnp.int32, (covs, covs), 0)
        == lax.broadcasted_iota(jnp.int32, (covs, covs), 1)
    ).astype(jnp.float32)
    covt = dot(eye, cov, 1, 1)
    solve = dot(cov, inverse(dot(covt, cov, 1, 0)), 1, 0)

    def blk_z(o, dev):
        return remote(blocks.at[o], blocks.at[o], z_send.at[dev // (cs * ys)], blk_recv.at[o], dev)

    def blk_y(o, dev):
        return remote(blocks.at[o], blocks.at[o], y_send.at[o], blk_recv.at[o], dev)

    def blk_c(o, dev):
        return remote(blocks.at[o], blocks.at[o], c_send.at[o], blk_recv.at[o], dev)

    y_dev = index(z, lax.rem(y + 1, ys), c)
    c_dev = index(z, y, lax.rem(c + 1, cs))

    @pl.when(me < nb)
    def _():
        raw[row_slice(me), :] = pheno_ref[:, lane_slice(me * LANES, LANES)]
        others(lambda src: raw_copy(src, me).wait_recv())
        pheno = raw[...]
        resid = pheno - dot(solve, dot(covt, pheno, 1, 0), 1, 0)
        var = jnp.sum(resid * resid, axis=0, keepdims=True) / samples + 0.1
        inv = 1.0 / var
        hi = inv.astype(jnp.bfloat16)
        rest = inv - hi.astype(jnp.float32)
        mid = rest.astype(jnp.bfloat16)
        low = (rest - mid.astype(jnp.float32)).astype(jnp.bfloat16)
        line = lax.broadcasted_iota(jnp.int32, (16, LANES), 0)
        extra = jnp.where(
            line == 0, hi.astype(jnp.float32),
            jnp.where(line == 1, mid.astype(jnp.float32),
                      jnp.where(line == 2, low.astype(jnp.float32), 0.0)),
        )
        blocks[me, pl.ds(samples, 16), :] = extra.astype(jnp.bfloat16)
        blocks[me, pl.ds(0, samples), :] = resid.astype(jnp.bfloat16)
        for k in range(1, zs):
            blk_z(me, index(lax.rem(z + k, zs), y, c)).start()
        if ys > 1:
            blk_y(me, y_dev).start()
        if cs > 1:
            blk_c(me, c_dev).start()

    others(lambda src: dose_copy(src, me).wait_recv())
    dose = dose_all[...].astype(jnp.float32).T
    dose = dose - dot(dot(dose, cov, 1, 0), solve, 1, 1)
    doset[...] = dose.astype(jnp.bfloat16)
    dose_var = jnp.sum(dose * dose, axis=1, keepdims=True) / samples + 0.1
    scale[...] = jnp.broadcast_to(1.0 / (samples * dose_var), scale.shape)

    def compute(o):
        extra = blocks[o, pl.ds(samples, 16), :].astype(jnp.float32)
        gene_scale = jnp.sum(extra[0:3, :], axis=0, keepdims=True)
        cross = dot(doset[...], blocks[o, pl.ds(0, samples), :], 1, 0, None)
        chi = cross * cross * (scale[...] * gene_scale)
        hit = 1.0 / (1.0 + jnp.exp(-2.0 * (chi - 4.0)))
        cols = lane_slice(o * LANES, LANES)
        part[0:1, cols] = jnp.sum(chi, axis=0, keepdims=True)
        part[1:2, cols] = jnp.sum(hit, axis=0, keepdims=True)

    @pl.when(me < nb)
    def _():
        compute(me)

    @pl.loop(1, zs)
    def _(k):
        o = index(lax.rem(z + k, zs), y, c)

        @pl.when(o < nb)
        def _():
            blk_z(o, me).wait_recv()
            if ys > 1:
                blk_y(o, y_dev).start()
            if cs > 1:
                blk_c(o, c_dev).start()
            compute(o)

    if ys > 1:
        @pl.loop(0, zs)
        def _(k):
            o = index(lax.rem(z + k, zs), lax.rem(y + 1, ys), c)

            @pl.when(o < nb)
            def _():
                blk_y(o, me).wait_recv()
                if cs > 1:
                    blk_c(o, c_dev).start()
                compute(o)

    if cs > 1:
        for j in range(ys):
            @pl.loop(0, zs)
            def _(k):
                o = index(lax.rem(z + k, zs), lax.rem(y + j, ys), lax.rem(c + 1, cs))

                @pl.when(o < nb)
                def _():
                    blk_c(o, me).wait_recv()
                    compute(o)

    window = landed.shape[2]

    def first(dev):
        return jnp.minimum(own * dev // LANES * LANES, genes - window)

    def part_copy(src, dev):
        return remote(
            part.at[:, lane_slice(first(dev), window)], landed.at[src],
            part_send.at[dev], part_recv.at[src], dev,
        )

    others(lambda dev: part_copy(me, dev).start())
    landed[me] = part[:, lane_slice(first(me), window)]
    others(lambda src: part_copy(src, me).wait_recv())
    total = jnp.sum(landed[...], axis=0)
    shift = own * me - first(me)
    out_ref[...] = pltpu.roll(total, lax.rem(window - shift, window), 1)

    def drain(dev):
        cov_copy(me, dev).wait_send()
        dose_copy(me, dev).wait_send()
        part_copy(me, dev).wait_send()

        @pl.when(dev < nb)
        def _():
            raw_copy(me, dev).wait_send()

    others(drain)

    @pl.when(me < nb)
    def _():
        for k in range(1, zs):
            blk_z(me, index(lax.rem(z + k, zs), y, c)).wait_send()

    @pl.loop(0, zs)
    def _(k):
        o = index(lax.rem(z + k, zs), y, c)

        @pl.when(o < nb)
        def _():
            if ys > 1:
                blk_y(o, y_dev).wait_send()
            if cs > 1:
                blk_c(o, c_dev).wait_send()

        if ys > 1 and cs > 1:
            other = index(lax.rem(z + k, zs), lax.rem(y + 1, ys), c)

            @pl.when(other < nb)
            def _():
                blk_c(other, c_dev).wait_send()


def local(dosage, covars, phenotypes):
    n = lax.axis_size("tile")
    rows, variants = dosage.shape
    genes = phenotypes.shape[1]
    covs = covars.shape[1]
    samples = rows * n
    cs = 2 if n % 2 == 0 else 1
    ys = 2 if n % (2 * cs) == 0 else 1
    zs = n // (cs * ys)
    nb = genes // LANES
    own = genes // n
    width = variants // n
    window = (own + LANES - 1 + LANES - 1) // LANES * LANES
    dma = pltpu.SemaphoreType.DMA
    out = pl.pallas_call(
        functools.partial(kernel, n, zs, ys, cs, own),
        out_shape=jax.ShapeDtypeStruct((8, window), jnp.float32),
        in_specs=[pl.BlockSpec(memory_space=pltpu.VMEM)] * 3,
        out_specs=pl.BlockSpec(memory_space=pltpu.VMEM),
        scratch_shapes=[
            pltpu.VMEM((n, 8, LANES), jnp.float32),
            pltpu.VMEM((samples, LANES), jnp.float32),
            pltpu.VMEM((samples, width), jnp.bfloat16),
            pltpu.VMEM((nb, samples + 16, LANES), jnp.bfloat16),
            pltpu.VMEM((width, samples), jnp.bfloat16),
            pltpu.VMEM((width, LANES), jnp.float32),
            pltpu.VMEM((8, genes), jnp.float32),
            pltpu.VMEM((n, 8, window), jnp.float32),
            pltpu.VMEM((8, LANES), jnp.float32),
            dma((n,)), dma((n,)), dma((n,)), dma((n,)), dma((n,)), dma((n,)),
            dma((zs,)), dma((nb,)), dma((nb,)), dma((nb,)), dma((n,)), dma((n,)),
        ],
        compiler_params=pltpu.CompilerParams(collective_id=0, has_side_effects=True),
    )(dosage, covars, phenotypes)
    return out[0, :own] / variants, 20.0 / variants * out[1, :own]


def solution(mesh):
    spec = P(("cohort", "tile"), None)
    return jax.shard_map(
        local,
        mesh=mesh,
        in_specs=(spec, spec, spec),
        out_specs=(P(("cohort", "tile")), P(("cohort", "tile"))),
        check_vma=False,
    )
```

```python
import functools

import jax
import jax.numpy as jnp
from jax import lax
from jax.experimental import pallas as pl
from jax.experimental.pallas import tpu as pltpu
from jax.sharding import PartitionSpec as P

LANES = 128
HIGH = lax.Precision.HIGHEST


def dot(a, b, ca, cb, precision=HIGH):
    return lax.dot_general(
        a, b, (((ca,), (cb,)), ((), ())), precision=precision, preferred_element_type=jnp.float32
    )


def inverse(gram):
    size = gram.shape[0]
    row_id = lax.broadcasted_iota(jnp.int32, (size, 2 * size), 0)
    eye = (
        lax.broadcasted_iota(jnp.int32, (size, size), 0)
        == lax.broadcasted_iota(jnp.int32, (size, size), 1)
    ).astype(jnp.float32)
    work = jnp.concatenate([gram, eye], axis=1)
    for k in range(size):
        row = work[k : k + 1, :] / work[k : k + 1, k : k + 1]
        work = jnp.where(row_id == k, row, work - work[:, k : k + 1] * row)
    return work[:, size:]


def kernel(
    n, zs, ys, cs, own,
    dose_in, cov_in, pheno_in, out_ref,
    dose_ref, cov_ref, pheno_ref, load_sem,
    cov_all, raw, dose_all, blocks, doset, scale, part, landed,
    cov_own, cov_send, cov_recv, raw_send, raw_recv, dose_send, dose_recv,
    z_send, pass_send, c_send, blk_recv, part_send, part_recv,
):
    me = lax.axis_index("tile")
    rows, variants = dose_ref.shape
    covs = cov_ref.shape[1]
    genes = pheno_ref.shape[1]
    nb = genes // (ys * LANES)
    peers = zs * cs
    width = variants // peers
    samples = rows * n
    c = lax.rem(me, cs)
    y = lax.rem(me // cs, ys)
    z = me // (cs * ys)
    place = z * cs + c

    def index(zi, yi, ci):
        return (zi * ys + yi) * cs + ci

    def place_of(t):
        return t // (cs * ys) * cs + lax.rem(t, cs)

    def at_place(p):
        return index(p // cs, y, lax.rem(p, cs))

    def remote(src, dst, ssem, rsem, dev):
        return pltpu.make_async_remote_copy(
            src_ref=src, dst_ref=dst, send_sem=ssem, recv_sem=rsem,
            device_id={"tile": dev}, device_id_type=pl.DeviceIdType.MESH,
        )

    def row_slice(t):
        return pl.ds(pl.multiple_of(t * rows, rows), rows)

    def lane_slice(start, size):
        return pl.ds(pl.multiple_of(start, LANES), size)

    cov_load = pltpu.make_async_copy(cov_in, cov_ref, load_sem.at[0])
    pheno_load = pltpu.make_async_copy(pheno_in, pheno_ref, load_sem.at[1])
    dose_load = pltpu.make_async_copy(dose_in, dose_ref, load_sem.at[2])
    barrier = pltpu.get_barrier_semaphore()
    for k in range(1, n):
        pl.semaphore_signal(
            barrier, inc=1, device_id={"tile": lax.rem(me + k, n)},
            device_id_type=pl.DeviceIdType.MESH,
        )
    cov_load.start()
    pheno_load.start()
    dose_load.start()
    cov_load.wait()
    groups = rows // 8
    packed = [cov_ref[8 * g : 8 * g + 8, :] for g in range(groups)]
    fill = jnp.zeros((8, LANES - groups * covs), jnp.float32)
    cov_own[...] = jnp.concatenate(packed + [fill], axis=1)
    pheno_load.wait()
    dose_load.wait()
    pl.semaphore_wait(barrier, n - 1)

    def cov_copy(src, dev):
        return remote(cov_own, cov_all.at[src], cov_send.at[dev], cov_recv.at[src], dev)

    def raw_copy(src, dev):
        return remote(
            pheno_ref.at[:, lane_slice((lax.rem(dev // cs, ys) * nb + place_of(dev)) * LANES, LANES)],
            raw.at[row_slice(src), :], raw_send.at[dev], raw_recv.at[src], dev,
        )

    def dose_copy(src, dev):
        return remote(
            dose_ref.at[:, lane_slice(place_of(dev) * width, width)],
            dose_all.at[row_slice(src), :], dose_send.at[dev], dose_recv.at[src], dev,
        )

    def others(body):
        @pl.loop(1, n)
        def _(k):
            body(lax.rem(me + k, n))

    others(lambda dev: cov_copy(me, dev).start())

    def send_first(dev):
        @pl.when(place_of(dev) < nb)
        def _():
            raw_copy(me, dev).start()

    def group(body):
        @pl.loop(1, peers)
        def _(k):
            body(at_place(lax.rem(place + k, peers)))

    y_dev = index(z, lax.rem(y + 1, ys), c)
    c_dev = index(z, y, lax.rem(c + 1, cs))

    def dose_pass(src):
        return remote(
            dose_all.at[row_slice(src), :], dose_all.at[row_slice(src), :],
            pass_send.at[src], dose_recv.at[src], y_dev,
        )

    others(send_first)
    group(lambda dev: dose_copy(me, dev).start())
    if ys > 1:
        dose_copy(me, y_dev).start()

    cov_all[me] = cov_own[...]
    dose_all[row_slice(me), :] = dose_ref[:, lane_slice(place * width, width)]

    others(lambda src: cov_copy(src, me).wait_recv())
    tiles = cov_all[...]
    cov = jnp.concatenate(
        [tiles[:, :, g * covs : (g + 1) * covs] for g in range(groups)], axis=1
    ).reshape(samples, covs)
    eye = (
        lax.broadcasted_iota(jnp.int32, (covs, covs), 0)
        == lax.broadcasted_iota(jnp.int32, (covs, covs), 1)
    ).astype(jnp.float32)
    covt = dot(eye, cov, 1, 1)
    solve = dot(cov, inverse(dot(covt, cov, 1, 0)), 1, 0)

    def blk_z(o, dev):
        return remote(blocks.at[o], blocks.at[o], z_send.at[dev // (cs * ys)], blk_recv.at[o], dev)

    def blk_c(o, dev):
        return remote(blocks.at[o], blocks.at[o], c_send.at[o], blk_recv.at[o], dev)

    @pl.when(place < nb)
    def _():
        raw[row_slice(me), :] = pheno_ref[:, lane_slice((y * nb + place) * LANES, LANES)]
        others(lambda src: raw_copy(src, me).wait_recv())
        pheno = raw[...]
        resid = pheno - dot(solve, dot(covt, pheno, 1, 0), 1, 0)
        var = jnp.sum(resid * resid, axis=0, keepdims=True) / samples + 0.1
        inv = 1.0 / var
        hi = inv.astype(jnp.bfloat16)
        rest = inv - hi.astype(jnp.float32)
        mid = rest.astype(jnp.bfloat16)
        low = (rest - mid.astype(jnp.float32)).astype(jnp.bfloat16)
        line = lax.broadcasted_iota(jnp.int32, (16, LANES), 0)
        extra = jnp.where(
            line == 0, hi.astype(jnp.float32),
            jnp.where(line == 1, mid.astype(jnp.float32),
                      jnp.where(line == 2, low.astype(jnp.float32), 0.0)),
        )
        blocks[place, pl.ds(samples, 16), :] = extra.astype(jnp.bfloat16)
        blocks[place, pl.ds(0, samples), :] = resid.astype(jnp.bfloat16)
        for k in range(1, zs):
            blk_z(place, index(lax.rem(z + k, zs), y, c)).start()
        if cs > 1:
            blk_c(place, c_dev).start()

    def hand_on(src):
        dose_copy(src, me).wait_recv()
        if ys > 1:
            dose_pass(src).start()

    group(hand_on)
    if ys > 1:
        @pl.loop(0, peers)
        def _(k):
            p = lax.rem(place + k, peers)
            src = index(p // cs, lax.rem(y + 1, ys), lax.rem(p, cs))
            dose_copy(src, me).wait_recv()

    dose = dose_all[...].astype(jnp.float32).T
    dose = dose - dot(dot(dose, cov, 1, 0), solve, 1, 1)
    doset[...] = dose.astype(jnp.bfloat16)
    dose_var = jnp.sum(dose * dose, axis=1, keepdims=True) / samples + 0.1
    scale[...] = jnp.broadcast_to(1.0 / (samples * dose_var), scale.shape)

    def compute(o):
        extra = blocks[o, pl.ds(samples, 16), :].astype(jnp.float32)
        gene_scale = jnp.sum(extra[0:3, :], axis=0, keepdims=True)
        cross = dot(doset[...], blocks[o, pl.ds(0, samples), :], 1, 0, None)
        chi = cross * cross * (scale[...] * gene_scale)
        hit = 1.0 / (1.0 + jnp.exp(-2.0 * (chi - 4.0)))
        cols = lane_slice(o * LANES, LANES)
        part[0:1, cols] = jnp.sum(chi, axis=0, keepdims=True)
        part[1:2, cols] = jnp.sum(hit, axis=0, keepdims=True)

    @pl.when(place < nb)
    def _():
        compute(place)

    @pl.loop(1, zs)
    def _(k):
        o = lax.rem(z + k, zs) * cs + c

        @pl.when(o < nb)
        def _():
            blk_z(o, me).wait_recv()
            if cs > 1:
                blk_c(o, c_dev).start()
            compute(o)

    if cs > 1:
        @pl.loop(0, zs)
        def _(k):
            o = lax.rem(z + k, zs) * cs + lax.rem(c + 1, cs)

            @pl.when(o < nb)
            def _():
                blk_c(o, me).wait_recv()
                compute(o)

    window = landed.shape[2]

    def owner(k):
        return y * peers + lax.rem(place + k, peers)

    def first(dev):
        return jnp.minimum(own * lax.rem(dev, peers) // LANES * LANES, nb * LANES - window)

    def part_copy(src, dev):
        return remote(
            part.at[:, lane_slice(first(dev), window)], landed.at[place_of(src)],
            part_send.at[lax.rem(dev, peers)], part_recv.at[place_of(src)], dev,
        )

    def each_part(body):
        @pl.loop(0, peers)
        def _(k):
            dev = owner(k)

            @pl.when(dev != me)
            def _():
                body(dev)

    def each_source(body):
        @pl.loop(0, peers)
        def _(k):
            src = index(k // cs, me // peers, lax.rem(k, cs))

            @pl.when(src != me)
            def _():
                body(src)

    each_part(lambda dev: part_copy(me, dev).start())

    @pl.when(me // peers == y)
    def _():
        landed[place] = part[:, lane_slice(first(me), window)]

    each_source(lambda src: part_copy(src, me).wait_recv())
    total = jnp.sum(landed[...], axis=0)
    shift = own * lax.rem(me, peers) - first(me)
    out_ref[...] = pltpu.roll(total, lax.rem(window - shift, window), 1)

    def drain(dev):
        cov_copy(me, dev).wait_send()

        @pl.when(place_of(dev) < nb)
        def _():
            raw_copy(me, dev).wait_send()

    others(drain)

    def drain_dose(dev):
        dose_copy(me, dev).wait_send()
        if ys > 1:
            dose_pass(dev).wait_send()

    group(drain_dose)
    if ys > 1:
        dose_copy(me, y_dev).wait_send()
    each_part(lambda dev: part_copy(me, dev).wait_send())

    @pl.when(place < nb)
    def _():
        for k in range(1, zs):
            blk_z(place, index(lax.rem(z + k, zs), y, c)).wait_send()

    if cs > 1:
        @pl.loop(0, zs)
        def _(k):
            o = lax.rem(z + k, zs) * cs + c

            @pl.when(o < nb)
            def _():
                blk_c(o, c_dev).wait_send()


def local(dosage, covars, phenotypes):
    n = lax.axis_size("tile")
    rows, variants = dosage.shape
    genes = phenotypes.shape[1]
    covs = covars.shape[1]
    samples = rows * n
    cs = 2 if n % 2 == 0 else 1
    ys = 2 if n % (2 * cs) == 0 else 1
    zs = n // (cs * ys)
    peers = zs * cs
    nb = genes // (ys * LANES)
    own = genes // n
    width = variants // peers
    window = (own + LANES - 1 + LANES - 1) // LANES * LANES
    dma = pltpu.SemaphoreType.DMA
    out = pl.pallas_call(
        functools.partial(kernel, n, zs, ys, cs, own),
        out_shape=jax.ShapeDtypeStruct((8, window), jnp.float32),
        in_specs=[pl.BlockSpec(memory_space=pl.ANY)] * 3,
        out_specs=pl.BlockSpec(memory_space=pltpu.VMEM),
        scratch_shapes=[
            pltpu.VMEM(dosage.shape, dosage.dtype),
            pltpu.VMEM(covars.shape, covars.dtype),
            pltpu.VMEM(phenotypes.shape, phenotypes.dtype),
            dma((3,)),
            pltpu.VMEM((n, 8, LANES), jnp.float32),
            pltpu.VMEM((samples, LANES), jnp.float32),
            pltpu.VMEM((samples, width), jnp.bfloat16),
            pltpu.VMEM((nb, samples + 16, LANES), jnp.bfloat16),
            pltpu.VMEM((width, samples), jnp.bfloat16),
            pltpu.VMEM((width, LANES), jnp.float32),
            pltpu.VMEM((8, nb * LANES), jnp.float32),
            pltpu.VMEM((peers, 8, window), jnp.float32),
            pltpu.VMEM((8, LANES), jnp.float32),
            dma((n,)), dma((n,)), dma((n,)), dma((n,)), dma((n,)), dma((n,)),
            dma((zs,)), dma((n,)), dma((nb,)), dma((nb,)), dma((peers,)), dma((peers,)),
        ],
        compiler_params=pltpu.CompilerParams(collective_id=0, has_side_effects=True),
    )(dosage, covars, phenotypes)
    return out[0, :own] / variants, 20.0 / variants * out[1, :own]


def solution(mesh):
    spec = P(("cohort", "tile"), None)
    return jax.shard_map(
        local,
        mesh=mesh,
        in_specs=(spec, spec, spec),
        out_specs=(P(("cohort", "tile")), P(("cohort", "tile"))),
        check_vma=False,
    )
```

```python
import functools

import jax
import jax.numpy as jnp
from jax import lax
from jax.experimental import pallas as pl
from jax.experimental.pallas import tpu as pltpu
from jax.sharding import PartitionSpec as P

LANES = 128
HIGH = lax.Precision.HIGHEST


def dot(a, b, ca, cb, precision=HIGH):
    return lax.dot_general(
        a, b, (((ca,), (cb,)), ((), ())), precision=precision, preferred_element_type=jnp.float32
    )


def inverse(gram):
    size = gram.shape[0]
    row_id = lax.broadcasted_iota(jnp.int32, (size, 2 * size), 0)
    eye = (
        lax.broadcasted_iota(jnp.int32, (size, size), 0)
        == lax.broadcasted_iota(jnp.int32, (size, size), 1)
    ).astype(jnp.float32)
    work = jnp.concatenate([gram, eye], axis=1)
    for k in range(size):
        row = work[k : k + 1, :] / work[k : k + 1, k : k + 1]
        work = jnp.where(row_id == k, row, work - work[:, k : k + 1] * row)
    return work[:, size:]


def kernel(
    n, zs, ys, cs, own,
    dose_in, cov_in, pheno_in, out_ref,
    dose_ref, cov_ref, pheno_ref, load_sem,
    cov_all, raw, dose_all, blocks, doset, scale, part, landed,
    cov_own, cov_send, cov_recv, raw_send, raw_recv, dose_send, dose_recv,
    z_send, pass_send, c_send, blk_recv, part_send, part_recv,
):
    me = lax.axis_index("tile")
    rows, variants = dose_ref.shape
    covs = cov_ref.shape[1]
    genes = pheno_ref.shape[1]
    nb = genes // (ys * LANES)
    peers = zs * cs
    width = variants // peers
    samples = rows * n
    c = lax.rem(me, cs)
    y = lax.rem(me // cs, ys)
    z = me // (cs * ys)
    place = z * cs + c

    def index(zi, yi, ci):
        return (zi * ys + yi) * cs + ci

    def place_of(t):
        return t // (cs * ys) * cs + lax.rem(t, cs)

    def at_place(p):
        return index(p // cs, y, lax.rem(p, cs))

    def remote(src, dst, ssem, rsem, dev):
        return pltpu.make_async_remote_copy(
            src_ref=src, dst_ref=dst, send_sem=ssem, recv_sem=rsem,
            device_id={"tile": dev}, device_id_type=pl.DeviceIdType.MESH,
        )

    def row_slice(t):
        return pl.ds(pl.multiple_of(t * rows, rows), rows)

    def lane_slice(start, size):
        return pl.ds(pl.multiple_of(start, LANES), size)

    cov_load = pltpu.make_async_copy(cov_in, cov_ref, load_sem.at[0])
    pheno_load = pltpu.make_async_copy(pheno_in, pheno_ref, load_sem.at[1])
    dose_load = pltpu.make_async_copy(dose_in, dose_ref, load_sem.at[2])
    barrier = pltpu.get_barrier_semaphore()
    for k in range(1, n):
        pl.semaphore_signal(
            barrier, inc=1, device_id={"tile": lax.rem(me + k, n)},
            device_id_type=pl.DeviceIdType.MESH,
        )
    cov_load.start()
    pheno_load.start()
    dose_load.start()
    cov_load.wait()
    groups = rows // 8
    packed = [cov_ref[8 * g : 8 * g + 8, :] for g in range(groups)]
    fill = jnp.zeros((8, LANES - groups * covs), jnp.float32)
    cov_own[...] = jnp.concatenate(packed + [fill], axis=1)
    pheno_load.wait()
    dose_load.wait()
    pl.semaphore_wait(barrier, n - 1)

    def cov_copy(src, dev):
        return remote(cov_own, cov_all.at[src], cov_send.at[dev], cov_recv.at[src], dev)

    def raw_copy(src, dev):
        return remote(
            pheno_ref.at[:, lane_slice((lax.rem(dev // cs, ys) * nb + place_of(dev)) * LANES, LANES)],
            raw.at[row_slice(src), :], raw_send.at[dev], raw_recv.at[src], dev,
        )

    def dose_copy(src, dev):
        return remote(
            dose_ref.at[:, lane_slice(place_of(dev) * width, width)],
            dose_all.at[row_slice(src), :], dose_send.at[dev], dose_recv.at[src], dev,
        )

    def others(body):
        @pl.loop(1, n)
        def _(k):
            body(lax.rem(me + k, n))

    others(lambda dev: cov_copy(me, dev).start())

    def send_first(dev):
        @pl.when(place_of(dev) < nb)
        def _():
            raw_copy(me, dev).start()

    def group(body):
        @pl.loop(1, peers)
        def _(k):
            body(at_place(lax.rem(place + k, peers)))

    y_dev = index(z, lax.rem(y + 1, ys), c)
    c_dev = index(z, y, lax.rem(c + 1, cs))

    def dose_pass(src):
        return remote(
            dose_all.at[row_slice(src), :], dose_all.at[row_slice(src), :],
            pass_send.at[src], dose_recv.at[src], y_dev,
        )

    others(send_first)
    group(lambda dev: dose_copy(me, dev).start())
    if ys > 1:
        dose_copy(me, y_dev).start()

    cov_all[me] = cov_own[...]
    dose_all[row_slice(me), :] = dose_ref[:, lane_slice(place * width, width)]

    others(lambda src: cov_copy(src, me).wait_recv())
    tiles = cov_all[...]
    cov = jnp.concatenate(
        [tiles[:, :, g * covs : (g + 1) * covs] for g in range(groups)], axis=1
    ).reshape(samples, covs)
    eye = (
        lax.broadcasted_iota(jnp.int32, (covs, covs), 0)
        == lax.broadcasted_iota(jnp.int32, (covs, covs), 1)
    ).astype(jnp.float32)
    covt = dot(eye, cov, 1, 1)
    solve = dot(cov, inverse(dot(covt, cov, 1, 0)), 1, 0)
    solve_parts = jnp.concatenate([solve] * 3, axis=1)
    cov_hi = cov.astype(jnp.bfloat16)
    cov_rest = cov - cov_hi.astype(jnp.float32)
    cov_mid = cov_rest.astype(jnp.bfloat16)
    cov_low = cov_rest - cov_mid.astype(jnp.float32)
    cov_parts = jnp.concatenate(
        [cov_hi.astype(jnp.float32), cov_mid.astype(jnp.float32), cov_low], axis=1
    ).astype(jnp.bfloat16)

    def blk_z(o, dev):
        return remote(blocks.at[o], blocks.at[o], z_send.at[dev // (cs * ys)], blk_recv.at[o], dev)

    def blk_c(o, dev):
        return remote(blocks.at[o], blocks.at[o], c_send.at[o], blk_recv.at[o], dev)

    @pl.when(place < nb)
    def _():
        raw[row_slice(me), :] = pheno_ref[:, lane_slice((y * nb + place) * LANES, LANES)]
        others(lambda src: raw_copy(src, me).wait_recv())
        pheno = raw[...]
        resid = pheno - dot(solve, dot(covt, pheno, 1, 0), 1, 0)
        var = jnp.sum(resid * resid, axis=0, keepdims=True) / samples + 0.1
        inv = 1.0 / var
        hi = inv.astype(jnp.bfloat16)
        rest = inv - hi.astype(jnp.float32)
        mid = rest.astype(jnp.bfloat16)
        low = (rest - mid.astype(jnp.float32)).astype(jnp.bfloat16)
        line = lax.broadcasted_iota(jnp.int32, (16, LANES), 0)
        extra = jnp.where(
            line == 0, hi.astype(jnp.float32),
            jnp.where(line == 1, mid.astype(jnp.float32),
                      jnp.where(line == 2, low.astype(jnp.float32), 0.0)),
        )
        blocks[place, pl.ds(samples, 16), :] = extra.astype(jnp.bfloat16)
        blocks[place, pl.ds(0, samples), :] = resid.astype(jnp.bfloat16)
        for k in range(1, zs):
            blk_z(place, index(lax.rem(z + k, zs), y, c)).start()
        if cs > 1:
            blk_c(place, c_dev).start()

    def hand_on(src):
        dose_copy(src, me).wait_recv()
        if ys > 1:
            dose_pass(src).start()

    group(hand_on)
    if ys > 1:
        @pl.loop(0, peers)
        def _(k):
            p = lax.rem(place + k, peers)
            src = index(p // cs, lax.rem(y + 1, ys), lax.rem(p, cs))
            dose_copy(src, me).wait_recv()

    dose_bf = dose_all[...].T
    cov_dose = dot(dose_bf, cov_parts, 1, 0, None)
    dose = dose_bf.astype(jnp.float32) - dot(cov_dose, solve_parts, 1, 1)
    doset[...] = dose.astype(jnp.bfloat16)
    dose_var = jnp.sum(dose * dose, axis=1, keepdims=True) / samples + 0.1
    scale[...] = jnp.broadcast_to(1.0 / (samples * dose_var), scale.shape)

    def compute(o):
        extra = blocks[o, pl.ds(samples, 16), :].astype(jnp.float32)
        gene_scale = jnp.sum(extra[0:3, :], axis=0, keepdims=True)
        cross = dot(doset[...], blocks[o, pl.ds(0, samples), :], 1, 0, None)
        chi = cross * cross * (scale[...] * gene_scale)
        hit = 1.0 / (1.0 + jnp.exp(-2.0 * (chi - 4.0)))
        cols = lane_slice(o * LANES, LANES)
        part[0:1, cols] = jnp.sum(chi, axis=0, keepdims=True)
        part[1:2, cols] = jnp.sum(hit, axis=0, keepdims=True)

    @pl.when(place < nb)
    def _():
        compute(place)

    @pl.loop(1, zs)
    def _(k):
        o = lax.rem(z + k, zs) * cs + c

        @pl.when(o < nb)
        def _():
            blk_z(o, me).wait_recv()
            if cs > 1:
                blk_c(o, c_dev).start()
            compute(o)

    if cs > 1:
        @pl.loop(0, zs)
        def _(k):
            o = lax.rem(z + k, zs) * cs + lax.rem(c + 1, cs)

            @pl.when(o < nb)
            def _():
                blk_c(o, me).wait_recv()
                compute(o)

    window = landed.shape[2]

    def owner(k):
        return y * peers + lax.rem(place + k, peers)

    def first(dev):
        return jnp.minimum(own * lax.rem(dev, peers) // LANES * LANES, nb * LANES - window)

    def part_copy(src, dev):
        return remote(
            part.at[:, lane_slice(first(dev), window)], landed.at[place_of(src)],
            part_send.at[lax.rem(dev, peers)], part_recv.at[place_of(src)], dev,
        )

    def each_part(body):
        @pl.loop(0, peers)
        def _(k):
            dev = owner(k)

            @pl.when(dev != me)
            def _():
                body(dev)

    def each_source(body):
        @pl.loop(0, peers)
        def _(k):
            src = index(k // cs, me // peers, lax.rem(k, cs))

            @pl.when(src != me)
            def _():
                body(src)

    each_part(lambda dev: part_copy(me, dev).start())

    @pl.when(me // peers == y)
    def _():
        landed[place] = part[:, lane_slice(first(me), window)]

    each_source(lambda src: part_copy(src, me).wait_recv())
    total = jnp.sum(landed[...], axis=0)
    shift = own * lax.rem(me, peers) - first(me)
    out_ref[...] = pltpu.roll(total, lax.rem(window - shift, window), 1)

    def drain(dev):
        cov_copy(me, dev).wait_send()

        @pl.when(place_of(dev) < nb)
        def _():
            raw_copy(me, dev).wait_send()

    others(drain)

    def drain_dose(dev):
        dose_copy(me, dev).wait_send()
        if ys > 1:
            dose_pass(dev).wait_send()

    group(drain_dose)
    if ys > 1:
        dose_copy(me, y_dev).wait_send()
    each_part(lambda dev: part_copy(me, dev).wait_send())

    @pl.when(place < nb)
    def _():
        for k in range(1, zs):
            blk_z(place, index(lax.rem(z + k, zs), y, c)).wait_send()

    if cs > 1:
        @pl.loop(0, zs)
        def _(k):
            o = lax.rem(z + k, zs) * cs + c

            @pl.when(o < nb)
            def _():
                blk_c(o, c_dev).wait_send()


def local(dosage, covars, phenotypes):
    n = lax.axis_size("tile")
    rows, variants = dosage.shape
    genes = phenotypes.shape[1]
    covs = covars.shape[1]
    samples = rows * n
    cs = 2 if n % 2 == 0 else 1
    ys = 2 if n % (2 * cs) == 0 else 1
    zs = n // (cs * ys)
    peers = zs * cs
    nb = genes // (ys * LANES)
    own = genes // n
    width = variants // peers
    window = (own + LANES - 1 + LANES - 1) // LANES * LANES
    dma = pltpu.SemaphoreType.DMA
    out = pl.pallas_call(
        functools.partial(kernel, n, zs, ys, cs, own),
        out_shape=jax.ShapeDtypeStruct((8, window), jnp.float32),
        in_specs=[pl.BlockSpec(memory_space=pl.ANY)] * 3,
        out_specs=pl.BlockSpec(memory_space=pltpu.VMEM),
        scratch_shapes=[
            pltpu.VMEM(dosage.shape, dosage.dtype),
            pltpu.VMEM(covars.shape, covars.dtype),
            pltpu.VMEM(phenotypes.shape, phenotypes.dtype),
            dma((3,)),
            pltpu.VMEM((n, 8, LANES), jnp.float32),
            pltpu.VMEM((samples, LANES), jnp.float32),
            pltpu.VMEM((samples, width), jnp.bfloat16),
            pltpu.VMEM((nb, samples + 16, LANES), jnp.bfloat16),
            pltpu.VMEM((width, samples), jnp.bfloat16),
            pltpu.VMEM((width, LANES), jnp.float32),
            pltpu.VMEM((8, nb * LANES), jnp.float32),
            pltpu.VMEM((peers, 8, window), jnp.float32),
            pltpu.VMEM((8, LANES), jnp.float32),
            dma((n,)), dma((n,)), dma((n,)), dma((n,)), dma((n,)), dma((n,)),
            dma((zs,)), dma((n,)), dma((nb,)), dma((nb,)), dma((peers,)), dma((peers,)),
        ],
        compiler_params=pltpu.CompilerParams(collective_id=0, has_side_effects=True),
    )(dosage, covars, phenotypes)
    return out[0, :own] / variants, 20.0 / variants * out[1, :own]


def solution(mesh):
    spec = P(("cohort", "tile"), None)
    return jax.shard_map(
        local,
        mesh=mesh,
        in_specs=(spec, spec, spec),
        out_specs=(P(("cohort", "tile")), P(("cohort", "tile"))),
        check_vma=False,
    )
```

```python
import functools

import jax
import jax.numpy as jnp
from jax import lax
from jax.experimental import pallas as pl
from jax.experimental.pallas import tpu as pltpu
from jax.sharding import PartitionSpec as P

LANES = 128
HIGH = lax.Precision.HIGHEST


def dot(a, b, ca, cb, precision=HIGH):
    return lax.dot_general(
        a, b, (((ca,), (cb,)), ((), ())), precision=precision, preferred_element_type=jnp.float32
    )


def inverse(gram):
    size = gram.shape[0]
    row_id = lax.broadcasted_iota(jnp.int32, (size, 2 * size), 0)
    eye = (
        lax.broadcasted_iota(jnp.int32, (size, size), 0)
        == lax.broadcasted_iota(jnp.int32, (size, size), 1)
    ).astype(jnp.float32)
    work = jnp.concatenate([gram, eye], axis=1)
    for k in range(size):
        row = work[k : k + 1, :] / work[k : k + 1, k : k + 1]
        work = jnp.where(row_id == k, row, work - work[:, k : k + 1] * row)
    return work[:, size:]


def partner(a, k, count):
    if count & (count - 1):
        return lax.rem(a + k, count)
    out, bit = 0, 1
    while bit < count:
        out = out + lax.rem(a // bit + k // bit, 2) * bit
        bit *= 2
    return out


def kernel(
    n, zs, ys, cs, own,
    dose_in, cov_in, pheno_in, out_ref,
    dose_ref, cov_ref, pheno_ref, load_sem,
    cov_all, raw, dose_all, blocks, doset, scale, part, landed,
    cov_own, cov_send, cov_recv, raw_send, raw_recv, dose_send, dose_recv,
    z_send, pass_send, c_send, blk_recv, part_send, part_recv,
):
    me = lax.axis_index("tile")
    rows, variants = dose_ref.shape
    covs = cov_ref.shape[1]
    genes = pheno_ref.shape[1]
    nb = genes // (ys * LANES)
    peers = zs * cs
    width = variants // peers
    samples = rows * n
    c = lax.rem(me, cs)
    y = lax.rem(me // cs, ys)
    z = me // (cs * ys)
    place = z * cs + c

    def index(zi, yi, ci):
        return (zi * ys + yi) * cs + ci

    def place_of(t):
        return t // (cs * ys) * cs + lax.rem(t, cs)

    def at_place(p):
        return index(p // cs, y, lax.rem(p, cs))

    def remote(src, dst, ssem, rsem, dev):
        return pltpu.make_async_remote_copy(
            src_ref=src, dst_ref=dst, send_sem=ssem, recv_sem=rsem,
            device_id={"tile": dev}, device_id_type=pl.DeviceIdType.MESH,
        )

    def row_slice(t):
        return pl.ds(pl.multiple_of(t * rows, rows), rows)

    def lane_slice(start, size):
        return pl.ds(pl.multiple_of(start, LANES), size)

    cov_load = pltpu.make_async_copy(cov_in, cov_ref, load_sem.at[0])
    pheno_load = pltpu.make_async_copy(pheno_in, pheno_ref, load_sem.at[1])
    dose_load = pltpu.make_async_copy(dose_in, dose_ref, load_sem.at[2])
    barrier = pltpu.get_barrier_semaphore()
    for k in range(1, n):
        pl.semaphore_signal(
            barrier, inc=1, device_id={"tile": lax.rem(me + k, n)},
            device_id_type=pl.DeviceIdType.MESH,
        )
    cov_load.start()
    pheno_load.start()
    dose_load.start()
    cov_load.wait()
    groups = rows // 8
    packed = [cov_ref[8 * g : 8 * g + 8, :] for g in range(groups)]
    fill = jnp.zeros((8, LANES - groups * covs), jnp.float32)
    cov_own[...] = jnp.concatenate(packed + [fill], axis=1)
    pheno_load.wait()
    dose_load.wait()
    pl.semaphore_wait(barrier, n - 1)

    def cov_copy(src, dev):
        return remote(cov_own, cov_all.at[src], cov_send.at[dev], cov_recv.at[src], dev)

    def raw_copy(src, dev):
        return remote(
            pheno_ref.at[:, lane_slice((lax.rem(dev // cs, ys) * nb + place_of(dev)) * LANES, LANES)],
            raw.at[row_slice(src), :], raw_send.at[dev], raw_recv.at[src], dev,
        )

    def dose_copy(src, dev):
        return remote(
            dose_ref.at[:, lane_slice(place_of(dev) * width, width)],
            dose_all.at[row_slice(src), :], dose_send.at[dev], dose_recv.at[src], dev,
        )

    def others(body):
        @pl.loop(1, n)
        def _(k):
            body(partner(me, k, n))

    others(lambda dev: cov_copy(me, dev).start())

    def send_first(dev):
        @pl.when(place_of(dev) < nb)
        def _():
            raw_copy(me, dev).start()

    def group(body):
        @pl.loop(1, peers)
        def _(k):
            body(at_place(partner(place, k, peers)))

    y_dev = index(z, lax.rem(y + 1, ys), c)
    c_dev = index(z, y, lax.rem(c + 1, cs))

    def dose_pass(src):
        return remote(
            dose_all.at[row_slice(src), :], dose_all.at[row_slice(src), :],
            pass_send.at[src], dose_recv.at[src], y_dev,
        )

    others(send_first)
    group(lambda dev: dose_copy(me, dev).start())
    if ys > 1:
        dose_copy(me, y_dev).start()

    cov_all[me] = cov_own[...]
    dose_all[row_slice(me), :] = dose_ref[:, lane_slice(place * width, width)]

    others(lambda src: cov_copy(src, me).wait_recv())
    tiles = cov_all[...]
    cov = jnp.concatenate(
        [tiles[:, :, g * covs : (g + 1) * covs] for g in range(groups)], axis=1
    ).reshape(samples, covs)
    eye = (
        lax.broadcasted_iota(jnp.int32, (covs, covs), 0)
        == lax.broadcasted_iota(jnp.int32, (covs, covs), 1)
    ).astype(jnp.float32)
    covt = dot(eye, cov, 1, 1)
    solve = dot(cov, inverse(dot(covt, cov, 1, 0)), 1, 0)
    solve_parts = jnp.concatenate([solve] * 3, axis=1)
    cov_hi = cov.astype(jnp.bfloat16)
    cov_rest = cov - cov_hi.astype(jnp.float32)
    cov_mid = cov_rest.astype(jnp.bfloat16)
    cov_low = cov_rest - cov_mid.astype(jnp.float32)
    cov_parts = jnp.concatenate(
        [cov_hi.astype(jnp.float32), cov_mid.astype(jnp.float32), cov_low], axis=1
    ).astype(jnp.bfloat16)

    def blk_z(o, dev):
        return remote(blocks.at[o], blocks.at[o], z_send.at[dev // (cs * ys)], blk_recv.at[o], dev)

    def blk_c(o, dev):
        return remote(blocks.at[o], blocks.at[o], c_send.at[o], blk_recv.at[o], dev)

    @pl.when(place < nb)
    def _():
        raw[row_slice(me), :] = pheno_ref[:, lane_slice((y * nb + place) * LANES, LANES)]
        others(lambda src: raw_copy(src, me).wait_recv())
        pheno = raw[...]
        resid = pheno - dot(solve, dot(covt, pheno, 1, 0), 1, 0)
        var = jnp.sum(resid * resid, axis=0, keepdims=True) / samples + 0.1
        inv = 1.0 / var
        hi = inv.astype(jnp.bfloat16)
        rest = inv - hi.astype(jnp.float32)
        mid = rest.astype(jnp.bfloat16)
        low = (rest - mid.astype(jnp.float32)).astype(jnp.bfloat16)
        line = lax.broadcasted_iota(jnp.int32, (16, LANES), 0)
        extra = jnp.where(
            line == 0, hi.astype(jnp.float32),
            jnp.where(line == 1, mid.astype(jnp.float32),
                      jnp.where(line == 2, low.astype(jnp.float32), 0.0)),
        )
        blocks[place, pl.ds(samples, 16), :] = extra.astype(jnp.bfloat16)
        blocks[place, pl.ds(0, samples), :] = resid.astype(jnp.bfloat16)
        for k in range(1, zs):
            blk_z(place, index(partner(z, k, zs), y, c)).start()
        if cs > 1:
            blk_c(place, c_dev).start()

    def hand_on(src):
        dose_copy(src, me).wait_recv()
        if ys > 1:
            dose_pass(src).start()

    group(hand_on)
    if ys > 1:
        @pl.loop(0, peers)
        def _(k):
            p = partner(place, k, peers)
            src = index(p // cs, lax.rem(y + 1, ys), lax.rem(p, cs))
            dose_copy(src, me).wait_recv()

    dose_bf = dose_all[...].T
    cov_dose = dot(dose_bf, cov_parts, 1, 0, None)
    dose = dose_bf.astype(jnp.float32) - dot(cov_dose, solve_parts, 1, 1)
    doset[...] = dose.astype(jnp.bfloat16)
    dose_var = jnp.sum(dose * dose, axis=1, keepdims=True) / samples + 0.1
    scale[...] = jnp.broadcast_to(1.0 / (samples * dose_var), scale.shape)

    def compute(o):
        extra = blocks[o, pl.ds(samples, 16), :].astype(jnp.float32)
        gene_scale = jnp.sum(extra[0:3, :], axis=0, keepdims=True)
        cross = dot(doset[...], blocks[o, pl.ds(0, samples), :], 1, 0, None)
        chi = cross * cross * (scale[...] * gene_scale)
        hit = 1.0 / (1.0 + jnp.exp(-2.0 * (chi - 4.0)))
        cols = lane_slice(o * LANES, LANES)
        part[0:1, cols] = jnp.sum(chi, axis=0, keepdims=True)
        part[1:2, cols] = jnp.sum(hit, axis=0, keepdims=True)

    @pl.when(place < nb)
    def _():
        compute(place)

    @pl.loop(1, zs)
    def _(k):
        o = partner(z, k, zs) * cs + c

        @pl.when(o < nb)
        def _():
            blk_z(o, me).wait_recv()
            if cs > 1:
                blk_c(o, c_dev).start()
            compute(o)

    if cs > 1:
        @pl.loop(0, zs)
        def _(k):
            o = partner(z, k, zs) * cs + lax.rem(c + 1, cs)

            @pl.when(o < nb)
            def _():
                blk_c(o, me).wait_recv()
                compute(o)

    window = landed.shape[2]

    def owner(k):
        return y * peers + partner(place, k, peers)

    def first(dev):
        return jnp.minimum(own * lax.rem(dev, peers) // LANES * LANES, nb * LANES - window)

    def part_copy(src, dev):
        return remote(
            part.at[:, lane_slice(first(dev), window)], landed.at[place_of(src)],
            part_send.at[lax.rem(dev, peers)], part_recv.at[place_of(src)], dev,
        )

    def each_part(body):
        @pl.loop(0, peers)
        def _(k):
            dev = owner(k)

            @pl.when(dev != me)
            def _():
                body(dev)

    def each_source(body):
        @pl.loop(0, peers)
        def _(k):
            src = index(k // cs, me // peers, lax.rem(k, cs))

            @pl.when(src != me)
            def _():
                body(src)

    each_part(lambda dev: part_copy(me, dev).start())

    @pl.when(me // peers == y)
    def _():
        landed[place] = part[:, lane_slice(first(me), window)]

    each_source(lambda src: part_copy(src, me).wait_recv())
    total = jnp.sum(landed[...], axis=0)
    shift = own * lax.rem(me, peers) - first(me)
    out_ref[...] = pltpu.roll(total, lax.rem(window - shift, window), 1)

    def drain(dev):
        cov_copy(me, dev).wait_send()

        @pl.when(place_of(dev) < nb)
        def _():
            raw_copy(me, dev).wait_send()

    others(drain)

    def drain_dose(dev):
        dose_copy(me, dev).wait_send()
        if ys > 1:
            dose_pass(dev).wait_send()

    group(drain_dose)
    if ys > 1:
        dose_copy(me, y_dev).wait_send()
    each_part(lambda dev: part_copy(me, dev).wait_send())

    @pl.when(place < nb)
    def _():
        for k in range(1, zs):
            blk_z(place, index(partner(z, k, zs), y, c)).wait_send()

    if cs > 1:
        @pl.loop(0, zs)
        def _(k):
            o = partner(z, k, zs) * cs + c

            @pl.when(o < nb)
            def _():
                blk_c(o, c_dev).wait_send()


def local(dosage, covars, phenotypes):
    n = lax.axis_size("tile")
    rows, variants = dosage.shape
    genes = phenotypes.shape[1]
    covs = covars.shape[1]
    samples = rows * n
    cs = 2 if n % 2 == 0 else 1
    ys = 2 if n % (2 * cs) == 0 else 1
    zs = n // (cs * ys)
    peers = zs * cs
    nb = genes // (ys * LANES)
    own = genes // n
    width = variants // peers
    window = (own + LANES - 1 + LANES - 1) // LANES * LANES
    dma = pltpu.SemaphoreType.DMA
    out = pl.pallas_call(
        functools.partial(kernel, n, zs, ys, cs, own),
        out_shape=jax.ShapeDtypeStruct((2, window), jnp.float32),
        in_specs=[pl.BlockSpec(memory_space=pl.ANY)] * 3,
        out_specs=pl.BlockSpec(memory_space=pltpu.VMEM),
        scratch_shapes=[
            pltpu.VMEM(dosage.shape, dosage.dtype),
            pltpu.VMEM(covars.shape, covars.dtype),
            pltpu.VMEM(phenotypes.shape, phenotypes.dtype),
            dma((3,)),
            pltpu.VMEM((n, 8, LANES), jnp.float32),
            pltpu.VMEM((samples, LANES), jnp.float32),
            pltpu.VMEM((samples, width), jnp.bfloat16),
            pltpu.VMEM((nb, samples + 16, LANES), jnp.bfloat16),
            pltpu.VMEM((width, samples), jnp.bfloat16),
            pltpu.VMEM((width, LANES), jnp.float32),
            pltpu.VMEM((2, nb * LANES), jnp.float32),
            pltpu.VMEM((peers, 2, window), jnp.float32),
            pltpu.VMEM((8, LANES), jnp.float32),
            dma((n,)), dma((n,)), dma((n,)), dma((n,)), dma((n,)), dma((n,)),
            dma((zs,)), dma((n,)), dma((nb,)), dma((nb,)), dma((peers,)), dma((peers,)),
        ],
        compiler_params=pltpu.CompilerParams(collective_id=0, has_side_effects=True),
    )(dosage, covars, phenotypes)
    return out[0, :own] / variants, 20.0 / variants * out[1, :own]


def solution(mesh):
    spec = P(("cohort", "tile"), None)
    return jax.shard_map(
        local,
        mesh=mesh,
        in_specs=(spec, spec, spec),
        out_specs=(P(("cohort", "tile")), P(("cohort", "tile"))),
        check_vma=False,
    )
```
